256 devices in a mesh: pair: 32 (over z, x), aux: 8 (over y, core).
Axes of the slice: x: 4, y: 4, z: 8, core: 2. Of those that a mesh axis runs over, the one named last changes fastest.
Arguments:
- integrals: bfloat16 [98304, 12288], P('pair', 'aux'), may hold values from -0.15625 to 0.15625
- energy_gaps: float32 [98304], P('pair'), may hold values from 0.3 to 3
- trial_vectors: float32 [98304, 64], P('pair'), may hold values from -160 to 160
Outputs:
- sigma_vectors: float32 [98304, 64], P(('pair', 'aux'))
- subspace: float32 [64, 64], replicated
- residuals: float32 [98304, 64], P(('pair', 'aux'))
- residual_norms: float32 [64], replicated
The draws below stay inside these ranges and needn't reach their ends.
All inputs are finite; a program needn't handle non-finite values.
Results may differ from the reference program's by a relative error of at most 0.0052.
Values may be sent and summed in bfloat16 or wider, within the bound.
A program may use at most 64 MiB of HBM per device.

```python
import math
import jax
import jax.numpy as jnp
from jax import lax

NAUX = 12288
NVEC = 64
PAIRS = 98304


def draw_trial_vectors(key, part):
    key_entries = jax.random.fold_in(key, 11)
    key_rows = jax.random.fold_in(key, 12)
    key_columns = jax.random.fold_in(key, 13)
    positions = jnp.arange(PAIRS).astype(jnp.float32)
    growth = jnp.exp(jnp.log(3.0) * positions / PAIRS)
    row_scale = jnp.exp(jax.random.uniform(key_rows, (PAIRS,), jnp.float32, jnp.log(0.3), jnp.log(3.0)))
    entries = jnp.clip(jax.random.normal(key_entries, (PAIRS, NVEC), jnp.float32), -5.0, 5.0)
    column_scale = jnp.exp(jax.random.uniform(key_columns, (NVEC,), jnp.float32, jnp.log(0.3), jnp.log(3.0)))
    return (entries * (growth * row_scale)[:, None] * column_scale[None, :]).astype(jnp.float32)


def spiked(values, rng, source, target, blocks, factor):
    def block_of(dim):
        return (jnp.arange(values.shape[dim]) // (values.shape[dim] // blocks)).reshape((-1,) + (1,) * (values.ndim - 1 - dim))

    first = jax.random.permutation(rng, blocks)[block_of(target)]
    second = (block_of(target) + blocks // 2) % blocks
    return jnp.where((block_of(source) == first) | (block_of(source) == second), factor * values, values)


def block_levels(rng, extent, split, low, high):
    factor_of, own = 1.0, jax.random.fold_in(rng, 6)
    for dim, blocks in split:
        heights = jnp.exp(jax.random.uniform(jax.random.fold_in(own, dim), (blocks,), jnp.float32, low / len(split), high / len(split)))
        factor_of = factor_of * jnp.repeat(heights, extent[dim] // blocks).reshape([-1 if axis == dim else 1 for axis in range(len(extent))])
    return factor_of


def heavy_noise(rng, shape, spread, limit, pieces, heavy, held_as=jnp.bfloat16):
    values = spread * jax.random.normal(rng, shape, jnp.float32)
    if pieces:
        values = values * block_levels(rng, shape, pieces, -0.22, 0.18)
    return jnp.clip(spiked(values, jax.random.fold_in(rng, 3), *heavy), -limit, limit).astype(held_as)


def setup_inputs(seed: int = 0) -> dict:
    streams_of = jax.random.split(jax.random.key(seed), 4)
    return {
        "integrals": heavy_noise(streams_of[0], (PAIRS, NAUX), (1.0 / (PAIRS * NAUX) ** 0.25), 0.15625, ((0, 32), (1, 8)), (0, 1, 32, 2.75)),
        "energy_gaps": jnp.clip(jnp.exp(math.log(3.0) - 2.3025851 * jax.random.uniform(streams_of[1], (PAIRS,), jnp.float32) ** block_levels(streams_of[1], (PAIRS,), ((0, 32),), -0.2, 0.2)), 0.3, 3.0),
        "trial_vectors": draw_trial_vectors(jax.random.fold_in(streams_of[3], 71), 0),
    }


epsilon = 1e-06

def reference(integrals, energy_gaps, trial_vectors):
    trial_half = trial_vectors.astype(jnp.bfloat16)
    aux_totals = lax.dot_general(integrals, trial_half, (((0,), (0,)), ((), ())), preferred_element_type=jnp.float32)
    aux_half = aux_totals.astype(jnp.bfloat16)
    coupled = jnp.dot(integrals, aux_half, preferred_element_type=jnp.float32)
    sigma_vectors = energy_gaps[:, None] * trial_vectors + 2.0 * coupled
    subspace = lax.dot_general(trial_vectors, sigma_vectors, (((0,), (0,)), ((), ())), precision=lax.Precision.HIGHEST, preferred_element_type=jnp.float32) / PAIRS
    intersection = lax.optimization_barrier(jnp.sum(trial_vectors * trial_vectors, axis=0)) / PAIRS
    rayleigh = jnp.diagonal(subspace) / (intersection + epsilon)
    residuals = sigma_vectors - trial_vectors * rayleigh[None, :]
    residual_norms = jnp.sqrt(lax.optimization_barrier(jnp.sum(residuals * residuals, axis=0)) / PAIRS + epsilon)
    return (sigma_vectors, subspace, residuals, residual_norms)
```

```python
import functools

import jax
import jax.numpy as jnp
from jax import lax
from jax.experimental import pallas as pl
from jax.experimental.pallas import tpu as pltpu
from jax.sharding import Mesh
from jax.sharding import PartitionSpec as P

AXES = ("z", "x", "y", "c")
PAIR = ("z", "x")
AUX = ("y", "c")
EPSILON = 1e-06
PIECES = 4
F32 = jnp.float32
BF16 = jnp.bfloat16
NT = (((1,), (1,)), ((), ()))


def far_first(i, n):
    step = lax.div(i + 1, 2)
    return n // 2 + step * (1 - 2 * lax.rem(i, 2))


def kernel(
    sizes,
    integrals,
    gaps,
    trial,
    sigma,
    subspace,
    residuals,
    norms,
    held,
    v,
    g,
    vh,
    parts,
    parts_in,
    half,
    at,
    mx,
    mz,
    gram_out,
    gram_in,
    prows,
    terms,
    terms_in,
    naux,
    npair,
    sig,
    res,
    load_sem,
    small_load,
    out_sem,
    send_sem,
    recv_sem,
):
    nz, nx, ny, nc = sizes
    na, npairs = ny * nc, nz * nx
    vectors, rows = v.shape
    columns = held.shape[1]
    kz, cx = vectors // nz, columns // nx
    own, ka = rows // na, vectors // na
    total_pairs = float(rows * npairs)
    z, x, y, c = (lax.axis_index(n) for n in AXES)
    a = y * nc + c
    me = z * nx + x

    def pair_at(oz, ox):
        return {"z": lax.rem(z + oz, nz), "x": lax.rem(x + ox, nx), "y": y, "c": c}

    def aux_at(oy, oc):
        return {"z": z, "x": x, "y": lax.rem(y + oy, ny), "c": lax.rem(c + oc, nc)}

    def pair_far(t):
        return pair_at(far_first(lax.div(t, nx), nz), far_first(lax.rem(t, nx), nx))

    def aux_far(t):
        return aux_at(far_first(lax.div(t, nc), ny), far_first(lax.rem(t, nc), nc))

    def send(src, dst, k, to):
        pltpu.make_async_remote_copy(
            src_ref=src,
            dst_ref=dst,
            send_sem=send_sem.at[k],
            recv_sem=recv_sem.at[k],
            device_id=to,
            device_id_type=pl.DeviceIdType.MESH,
        ).start()

    def arrived(ref, k):
        pltpu.make_async_remote_copy(
            src_ref=ref,
            dst_ref=ref,
            send_sem=send_sem.at[k],
            recv_sem=recv_sem.at[k],
            device_id=pair_at(1, 0),
            device_id_type=pl.DeviceIdType.MESH,
        ).wait_recv()

    def sent(ref, k):
        pltpu.make_async_remote_copy(
            src_ref=ref,
            dst_ref=ref,
            send_sem=send_sem.at[k],
            recv_sem=recv_sem.at[k],
            device_id=pair_at(1, 0),
            device_id_type=pl.DeviceIdType.MESH,
        ).wait_send()

    def each(n, body):
        def step(i, carry):
            body(i)
            return carry

        lax.fori_loop(0, n, step, 0)

    load_v = pltpu.make_async_copy(trial, v, small_load.at[0])
    load_g = pltpu.make_async_copy(gaps, g, small_load.at[1])
    load_v.start()
    load_g.start()

    def columns_of(i):
        xx = lax.rem(x + far_first(i, nx), nx)
        return pl.ds(pl.multiple_of(xx * cx, 128), cx)

    piece = rows // PIECES

    def load_chunk(i):
        for p in range(PIECES):
            where = (pl.ds(p * piece, piece), columns_of(i))
            pltpu.make_async_copy(integrals.at[where], held.at[where], load_sem.at[i]).start()

    each(nx, load_chunk)

    barrier = pltpu.get_barrier_semaphore()

    def greet(to):
        pl.semaphore_signal(barrier, inc=1, device_id=to, device_id_type=pl.DeviceIdType.MESH)

    each(npairs - 1, lambda t: greet(pair_far(t)))
    each(na - 1, lambda t: greet(aux_far(t)))

    load_v.wait()
    load_g.wait()
    vh[...] = v[...].astype(BF16)

    def first_product(i):
        cols = columns_of(i)
        pltpu.make_async_copy(integrals.at[:, cols], held.at[:, cols], load_sem.at[i]).wait()
        part = jnp.dot(vh[...], held[:, cols], preferred_element_type=F32)
        parts[i] = part.astype(BF16).reshape(nz, kz, cx)

        @pl.when(i == 0)
        def _():
            pl.semaphore_wait(barrier, npairs - 1 + na - 1)

        def scatter(j):
            oz = far_first(j, nz)
            zz = lax.rem(z + oz, nz)
            to = pair_at(oz, far_first(i, nx))
            t = j * nx + i
            send(parts.at[i, zz], parts_in.at[t], 0, to)

        each(jnp.where(i == nx - 1, nz - 1, nz), scatter)

    each(nx, first_product)

    first = pl.multiple_of(a * ka, ka)
    mine = v[pl.ds(first, ka), :]
    gv = v[...] * g[...]
    m1 = lax.dot_general(mine, gv, NT, precision=lax.Precision.HIGHEST, preferred_element_type=F32)
    squares = jnp.sum(mine * mine, axis=1, keepdims=True)
    mx[x] = jnp.concatenate([m1, jnp.broadcast_to(squares, (ka, vectors))], axis=1)
    each(nx - 1, lambda t: send(mx.at[x], mx.at[x], 1, pair_at(0, far_first(t, nx))))

    arrived(parts_in, 0)
    block = parts[nx - 1, z].astype(F32)
    block = block + jnp.sum(parts_in[...].astype(F32), axis=0)
    slot = x * nz + z
    half[slot] = block.astype(BF16)
    each(npairs - 1, lambda t: send(half.at[slot], half.at[slot], 2, pair_far(t)))

    arrived(mx.at[pl.ds(0, nx - 1)], 1)
    mz[z] = jnp.sum(mx[...], axis=0)
    each(nz - 1, lambda t: send(mz.at[z], mz.at[z], 3, pair_at(far_first(t, nz), 0)))

    arrived(half.at[pl.ds(0, npairs - 1)], 2)
    for i in range(nx):
        at[:, i * cx : (i + 1) * cx] = half[i * nz : (i + 1) * nz].reshape(vectors, cx)

    gram = lax.dot_general(at[...], at[...], NT, preferred_element_type=F32)
    gram = jnp.concatenate([gram, jnp.zeros((vectors, 128 - vectors), F32)], axis=1)
    gram_out[...] = gram.reshape(na, ka, 128)

    def scatter_gram(t):
        to = aux_far(t)
        send(gram_out.at[to["y"] * nc + to["c"]], gram_in.at[a], 4, to)

    each(na - 1, scatter_gram)
    gram_in[a] = gram_out[a]

    def second_product(t):
        to = aux_far(t)
        begin = pl.multiple_of((to["y"] * nc + to["c"]) * own, own)
        out = lax.dot_general(at[...], held[pl.ds(begin, own), :], NT, preferred_element_type=F32)
        terms[t] = out.astype(BF16)
        send(terms.at[t], terms_in.at[t], 5, to)

    each(na - 1, second_product)

    arrived(mz.at[pl.ds(0, nz - 1)], 3)
    arrived(gram_in.at[pl.ds(0, na - 1)], 4)
    prows[a] = jnp.sum(mz[...], axis=0) + 2.0 * jnp.sum(gram_in[...], axis=0)
    each(na - 1, lambda t: send(prows.at[a], prows.at[a], 6, aux_far(t)))

    begin = pl.multiple_of(a * own, own)
    coupled = lax.dot_general(at[...], held[pl.ds(begin, own), :], NT, preferred_element_type=F32)
    mine_at = pl.ds(pl.multiple_of(a * own, 128), own)
    own_trial = v[:, mine_at]
    gapped = own_trial * g[:, mine_at]

    arrived(prows.at[pl.ds(0, na - 1)], 6)
    products = prows[...].reshape(vectors, 128)
    row = lax.broadcasted_iota(jnp.int32, (vectors, 128), 0)
    lane = lax.broadcasted_iota(jnp.int32, (vectors, 128), 1)
    sub = products / total_pairs
    diagonal = jnp.sum(jnp.where(row == lane, sub, 0.0), axis=1, keepdims=True)
    intersection = jnp.sum(jnp.where(lane == vectors, sub, 0.0), axis=1, keepdims=True)
    rayleigh = diagonal / (intersection + EPSILON)
    subspace[...] = sub[:, :vectors]

    arrived(terms_in, 5)
    coupled = coupled + jnp.sum(terms_in[...].astype(F32), axis=0)
    sigma_own = gapped + 2.0 * coupled
    sig[...] = sigma_own
    residual = sigma_own - rayleigh * own_trial
    res[...] = residual
    squared = residual * residual
    lanes = squared[:, :128]
    for i in range(1, own // 128):
        lanes = lanes + squared[:, i * 128 : (i + 1) * 128]
    lanes = jnp.concatenate([lanes, jnp.zeros((128 - vectors, 128), F32)], axis=0)
    naux[a] = jnp.sum(lanes.T, axis=0, keepdims=True)
    each(na - 1, lambda t: send(naux.at[a], naux.at[a], 7, aux_far(t)))
    put_sigma = pltpu.make_async_copy(sig, sigma, out_sem.at[0])
    put_residuals = pltpu.make_async_copy(res, residuals, out_sem.at[1])
    put_sigma.start()
    put_residuals.start()
    arrived(naux.at[pl.ds(0, na - 1)], 7)
    npair[me] = jnp.sum(naux[...], axis=0)
    each(npairs - 1, lambda t: send(npair.at[me], npair.at[me], 8, pair_far(t)))

    sent(parts_in, 0)
    sent(mx.at[pl.ds(0, nx - 1)], 1)
    sent(half.at[pl.ds(0, npairs - 1)], 2)
    sent(mz.at[pl.ds(0, nz - 1)], 3)
    sent(gram_in.at[pl.ds(0, na - 1)], 4)
    sent(terms_in, 5)
    sent(prows.at[pl.ds(0, na - 1)], 6)
    sent(naux.at[pl.ds(0, na - 1)], 7)
    put_sigma.wait()
    put_residuals.wait()
    arrived(npair.at[pl.ds(0, npairs - 1)], 8)
    sent(npair.at[pl.ds(0, npairs - 1)], 8)
    total = jnp.sum(npair[...], axis=0) / total_pairs
    norms[...] = jnp.sqrt(total[:, :vectors] + EPSILON)


def local(sizes, integrals, energy_gaps, trial_vectors):
    nz, nx, ny, nc = sizes
    na, npairs = ny * nc, nz * nx
    rows, columns = integrals.shape
    vectors = trial_vectors.shape[1]
    kz, cx = vectors // nz, columns // nx
    own, ka = rows // na, vectors // na
    hbm = pl.BlockSpec(memory_space=pl.ANY)
    vmem = pl.BlockSpec(memory_space=pltpu.VMEM)
    sigma, subspace, residuals, norms = pl.pallas_call(
        functools.partial(kernel, sizes),
        out_shape=(
            jax.ShapeDtypeStruct((vectors, own), F32),
            jax.ShapeDtypeStruct((vectors, vectors), F32),
            jax.ShapeDtypeStruct((vectors, own), F32),
            jax.ShapeDtypeStruct((1, vectors), F32),
        ),
        in_specs=[hbm, hbm, hbm],
        out_specs=(hbm, vmem, hbm, vmem),
        scratch_shapes=[
            pltpu.VMEM((rows, columns), BF16),
            pltpu.VMEM((vectors, rows), F32),
            pltpu.VMEM((1, rows), F32),
            pltpu.VMEM((vectors, rows), BF16),
            pltpu.VMEM((nx, nz, kz, cx), BF16),
            pltpu.VMEM((npairs - 1, kz, cx), BF16),
            pltpu.VMEM((npairs, kz, cx), BF16),
            pltpu.VMEM((vectors, columns), BF16),
            pltpu.VMEM((nx, ka, 128), F32),
            pltpu.VMEM((nz, ka, 128), F32),
            pltpu.VMEM((na, ka, 128), F32),
            pltpu.VMEM((na, ka, 128), F32),
            pltpu.VMEM((na, ka, 128), F32),
            pltpu.VMEM((na - 1, vectors, own), BF16),
            pltpu.VMEM((na - 1, vectors, own), BF16),
            pltpu.VMEM((na, 1, 128), F32),
            pltpu.VMEM((npairs, 1, 128), F32),
            pltpu.VMEM((vectors, own), F32),
            pltpu.VMEM((vectors, own), F32),
            pltpu.SemaphoreType.DMA((nx,)),
            pltpu.SemaphoreType.DMA((2,)),
            pltpu.SemaphoreType.DMA((2,)),
            pltpu.SemaphoreType.DMA((9,)),
            pltpu.SemaphoreType.DMA((9,)),
        ],
        compiler_params=pltpu.CompilerParams(
            collective_id=0, has_side_effects=True, vmem_limit_bytes=60 * 1024 * 1024
        ),
        name="sigma_build",
    )(integrals, energy_gaps.reshape(1, rows), trial_vectors.T)
    return sigma.T, subspace, residuals.T, norms.reshape(vectors)


def solution(mesh):
    sizes = (8, 4, 4, 2)
    finer = Mesh(mesh.devices.reshape(sizes), AXES)
    return build(finer, sizes)


def build(finer, sizes):
    return jax.shard_map(
        functools.partial(local, sizes),
        mesh=finer,
        in_specs=(P(PAIR, AUX), P(PAIR), P(PAIR, None)),
        out_specs=(P(PAIR + AUX, None), P(), P(PAIR + AUX, None), P()),
        check_vma=False,
    )
```

```python
import functools

import jax
import jax.numpy as jnp
from jax import lax
from jax.experimental import pallas as pl
from jax.experimental.pallas import tpu as pltpu
from jax.sharding import Mesh
from jax.sharding import PartitionSpec as P

AXES = ("z", "x", "y", "c")
PAIR = ("z", "x")
AUX = ("y", "c")
EPSILON = 1e-06
PIECES = 4
F32 = jnp.float32
BF16 = jnp.bfloat16
NT = (((1,), (1,)), ((), ()))


def farthest(n):
    return sorted(range(n), key=lambda d: -min(d, n - d))


def far_first(i, n):
    step = lax.div(i + 1, 2)
    return n // 2 + step * (1 - 2 * lax.rem(i, 2))


def kernel(
    sizes,
    integrals,
    gaps,
    trial,
    sigma,
    subspace,
    residuals,
    norms,
    held,
    v,
    g,
    vh,
    parts,
    parts_in,
    half,
    at,
    mx,
    mz,
    gc,
    gy,
    prows,
    terms,
    terms_in,
    coupled,
    nchip,
    nall,
    load_sem,
    small_load,
    terms_sem,
    send_sem,
    recv_sem,
):
    nz, nx, ny, nc = sizes
    na, npairs = ny * nc, nz * nx
    vectors, rows = v.shape
    columns = held.shape[1]
    kz, cx = vectors // nz, columns // nx
    own, ka = rows // na, vectors // na
    total_pairs = float(rows * npairs)
    z, x, y, c = (lax.axis_index(n) for n in AXES)
    a = y * nc + c
    me = z * nx + x

    zs, xs, ys, cs = ([lax.rem(p + d, n) for d in range(n)] for p, n in zip((z, x, y, c), sizes))
    plane = [(zs[i], xs[j], y, c) for i in farthest(nz) for j in farthest(nx)][:-1]
    group = [(z, x, ys[i], cs[j]) for i in farthest(ny) for j in reversed(range(nc))][:-1]
    sibling = (z, x, y, cs[1])
    y_others = [(z, x, ys[i], c) for i in farthest(ny)][:-1]
    x_others = [(z, xs[j], y, c) for j in farthest(nx)][:-1]
    z_others = [(zs[i], x, y, c) for i in farthest(nz)][:-1]

    def send(src, dst, k, to):
        pltpu.make_async_remote_copy(
            src_ref=src,
            dst_ref=dst,
            send_sem=send_sem.at[k],
            recv_sem=recv_sem.at[k],
            device_id=to,
            device_id_type=pl.DeviceIdType.MESH,
        ).start()

    def arrived(ref, k):
        pltpu.make_async_remote_copy(
            src_ref=ref,
            dst_ref=ref,
            send_sem=send_sem.at[k],
            recv_sem=recv_sem.at[k],
            device_id=sibling,
            device_id_type=pl.DeviceIdType.MESH,
        ).wait_recv()

    def sent(ref, k):
        pltpu.make_async_remote_copy(
            src_ref=ref,
            dst_ref=ref,
            send_sem=send_sem.at[k],
            recv_sem=recv_sem.at[k],
            device_id=sibling,
            device_id_type=pl.DeviceIdType.MESH,
        ).wait_send()

    def each(n, body):
        def step(i, carry):
            body(i)
            return carry

        lax.fori_loop(0, n, step, 0)

    load_v = pltpu.make_async_copy(trial, v, small_load.at[0])
    load_g = pltpu.make_async_copy(gaps, g, small_load.at[1])
    load_v.start()
    load_g.start()

    def columns_of(i):
        xx = lax.rem(x + far_first(i, nx), nx)
        return pl.ds(pl.multiple_of(xx * cx, 128), cx)

    piece = rows // PIECES

    def load_chunk(i):
        for p in range(PIECES):
            where = (pl.ds(p * piece, piece), columns_of(i))
            pltpu.make_async_copy(integrals.at[where], held.at[where], load_sem.at[i]).start()

    load_chunk(0)
    barrier = pltpu.get_barrier_semaphore()
    for to in plane + group:
        pl.semaphore_signal(barrier, inc=1, device_id=to, device_id_type=pl.DeviceIdType.MESH)
    for i in range(1, nx):
        load_chunk(i)

    load_v.wait()
    load_g.wait()
    vh[...] = v[...].astype(BF16)

    def scatter(i):
        xx = lax.rem(x + far_first(i, nx), nx)
        for j, oz in enumerate(farthest(nz)[:-1]):
            send(parts.at[i, zs[oz]], parts_in.at[j * nx + i], 0, (zs[oz], xx, y, c))

        @pl.when(i < nx - 1)
        def _():
            send(parts.at[i, z], parts_in.at[(nz - 1) * nx + i], 0, (z, xx, y, c))

    def first_product(i):
        cols = columns_of(i)
        pltpu.make_async_copy(integrals.at[:, cols], held.at[:, cols], load_sem.at[i]).wait()
        part = jnp.dot(vh[...], held[:, cols], preferred_element_type=F32)
        parts[i] = part.astype(BF16).reshape(nz, kz, cx)

        @pl.when(i == 1)
        def _():
            pl.semaphore_wait(barrier, len(plane) + len(group))
            scatter(0)

        @pl.when(i > 0)
        def _():
            scatter(i)

    each(nx, first_product)

    first = pl.multiple_of(a * ka, ka)
    mine = v[pl.ds(first, ka), :]
    gv = v[...] * g[...]
    m1 = lax.dot_general(mine, gv, NT, precision=lax.Precision.HIGHEST, preferred_element_type=F32)
    squares = jnp.sum(mine * mine, axis=1, keepdims=True)
    mx[x] = jnp.concatenate([m1, jnp.broadcast_to(squares, (ka, vectors))], axis=1)
    for to in x_others:
        send(mx.at[x], mx.at[x], 1, to)

    arrived(parts_in, 0)
    block = parts[nx - 1, z].astype(F32)
    block = block + jnp.sum(parts_in[...].astype(F32), axis=0)
    slot = x * nz + z
    half[slot] = block.astype(BF16)
    for to in plane:
        send(half.at[slot], half.at[slot], 2, to)

    arrived(mx.at[pl.ds(0, nx - 1)], 1)
    mz[z] = jnp.sum(mx[...], axis=0)
    for to in z_others:
        send(mz.at[z], mz.at[z], 3, to)

    arrived(half.at[pl.ds(0, npairs - 1)], 2)
    for i in range(nx):
        at[:, i * cx : (i + 1) * cx] = half[i * nz : (i + 1) * nz].reshape(vectors, cx)

    low = vectors // 2

    def second_product(i):
        yy = lax.rem(y + far_first(i, ny), ny)
        begin = pl.multiple_of(yy * nc * own, nc * own)
        out = lax.dot_general(at[...], held[pl.ds(begin, nc * own), :], NT, preferred_element_type=F32)
        for j in range(nc):
            terms[i, j] = out[:, j * own : (j + 1) * own].astype(BF16)

        def put(j, to):
            pltpu.make_async_remote_copy(
                src_ref=terms.at[i, j],
                dst_ref=terms_in.at[i, c],
                send_sem=send_sem.at[5],
                recv_sem=terms_sem.at[i, c],
                device_id=to,
                device_id_type=pl.DeviceIdType.MESH,
            ).start()

        @pl.when(i < ny - 1)
        def _():
            for j in range(nc):
                put(j, (z, x, yy, j))

        @pl.when(i == ny - 1)
        def _():
            put(cs[1], sibling)
            coupled[...] = jnp.where(c == 0, out[:, :own], out[:, own:])

        @pl.when(i == 0)
        def _():
            gram = lax.dot_general(at[...], at[...], NT, preferred_element_type=F32)
            gc[c] = jnp.concatenate([gram[:low], gram[low:]], axis=1)
            send(gc.at[c], gc.at[c], 4, sibling)

        @pl.when(i == ny - 2)
        def _():
            arrived(mz.at[pl.ds(0, nz - 1)], 3)
            prows[a] = jnp.sum(mz[...], axis=0)
            for to in group:
                send(prows.at[a], prows.at[a], 6, to)
            arrived(gc.at[0], 4)
            gy[y] = gc[0] + gc[1]
            for to in y_others:
                send(gy.at[y], gy.at[y], 7, to)

    each(ny, second_product)
    mine_at = pl.ds(pl.multiple_of(a * own, 128), own)
    own_trial = v[:, mine_at]

    arrived(prows.at[pl.ds(0, na - 1)], 6)
    arrived(gy.at[pl.ds(0, ny - 1)], 7)
    gram = jnp.sum(gy[...], axis=0)
    gram = jnp.concatenate([gram[:, :vectors], gram[:, vectors:]], axis=0)
    inputs = prows[...].reshape(vectors, 2 * vectors)
    sub = (inputs[:, :vectors] + 2.0 * gram) / total_pairs
    row = lax.broadcasted_iota(jnp.int32, (vectors, vectors), 0)
    lane = lax.broadcasted_iota(jnp.int32, (vectors, vectors), 1)
    diagonal = jnp.sum(jnp.where(row == lane, sub, 0.0), axis=1, keepdims=True)
    intersection = inputs[:, vectors : vectors + 1] / total_pairs
    rayleigh = diagonal / (intersection + EPSILON)
    subspace[...] = sub

    def arrived_term(i, j):
        pltpu.make_async_remote_copy(
            src_ref=terms.at[i, j],
            dst_ref=terms_in.at[i, j],
            send_sem=send_sem.at[5],
            recv_sem=terms_sem.at[i, j],
            device_id=sibling,
            device_id_type=pl.DeviceIdType.MESH,
        ).wait_recv()
        return terms_in[i, j].astype(F32)

    total = coupled[...] + arrived_term(ny - 1, cs[1])
    for i in range(ny - 1):
        for j in range(nc):
            total = total + arrived_term(i, j)

    sigma_own = own_trial * g[:, mine_at] + 2.0 * total
    sigma[...] = sigma_own
    residual = sigma_own - rayleigh * own_trial
    residuals[...] = residual
    squared = residual * residual
    lanes = squared[:, :128]
    for i in range(1, own // 128):
        lanes = lanes + squared[:, i * 128 : (i + 1) * 128]
    lanes = jnp.concatenate([lanes, jnp.zeros((128 - vectors, 128), F32)], axis=0)
    nchip[c] = jnp.sum(lanes.T, axis=0, keepdims=True)
    send(nchip.at[c], nchip.at[c], 8, sibling)

    arrived(nchip.at[0], 8)
    nall[me * ny + y] = nchip[0] + nchip[1]

    def share(t):
        zz = lax.rem(z + far_first(lax.div(t, nx), nz), nz)
        xx = lax.rem(x + far_first(lax.rem(t, nx), nx), nx)
        for k in farthest(ny)[:-1]:
            send(nall.at[me * ny + y], nall.at[me * ny + y], 9, (zz, xx, ys[k], c))

        @pl.when(t < npairs - 1)
        def _():
            send(nall.at[me * ny + y], nall.at[me * ny + y], 9, (zz, xx, y, c))

    each(npairs, share)

    sent(parts_in, 0)
    sent(mx.at[pl.ds(0, nx - 1)], 1)
    sent(half.at[pl.ds(0, npairs - 1)], 2)
    sent(mz.at[pl.ds(0, nz - 1)], 3)
    sent(gc.at[0], 4)
    sent(terms.at[pl.ds(0, ny - 1)], 5)
    sent(terms.at[0, 0], 5)
    sent(prows.at[pl.ds(0, na - 1)], 6)
    sent(gy.at[pl.ds(0, ny - 1)], 7)
    sent(nchip.at[0], 8)

    arrived(nall.at[pl.ds(0, npairs * ny - 1)], 9)
    sent(nall.at[pl.ds(0, npairs * ny - 1)], 9)
    total = jnp.sum(nall[...], axis=0) / total_pairs
    norms[...] = jnp.sqrt(total[:, :vectors] + EPSILON)


def put_out(*refs):
    copies = [pltpu.make_async_copy(refs[i], refs[4 + i], refs[8].at[i]) for i in range(4)]
    for copy in copies:
        copy.start()
    for copy in copies:
        copy.wait()


def local(sizes, integrals, energy_gaps, trial_vectors):
    nz, nx, ny, nc = sizes
    na, npairs = ny * nc, nz * nx
    rows, columns = integrals.shape
    vectors = trial_vectors.shape[1]
    kz, cx = vectors // nz, columns // nx
    own, ka = rows // na, vectors // na
    hbm = pl.BlockSpec(memory_space=pl.ANY)
    vmem = pl.BlockSpec(memory_space=pltpu.VMEM)
    shapes = ((vectors, own), (vectors, vectors), (vectors, own), (1, vectors))
    results = pl.pallas_call(
        functools.partial(kernel, sizes),
        out_shape=tuple(pltpu.VMEM(s, F32) for s in shapes),
        in_specs=[hbm, hbm, hbm],
        out_specs=(vmem,) * 4,
        scratch_shapes=[
            pltpu.VMEM((rows, columns), BF16),
            pltpu.VMEM((vectors, rows), F32),
            pltpu.VMEM((1, rows), F32),
            pltpu.VMEM((vectors, rows), BF16),
            pltpu.VMEM((nx, nz, kz, cx), BF16),
            pltpu.VMEM((npairs - 1, kz, cx), BF16),
            pltpu.VMEM((npairs, kz, cx), BF16),
            pltpu.VMEM((vectors, columns), BF16),
            pltpu.VMEM((nx, ka, 128), F32),
            pltpu.VMEM((nz, ka, 128), F32),
            pltpu.VMEM((nc, vectors // 2, 2 * vectors), F32),
            pltpu.VMEM((ny, vectors // 2, 2 * vectors), F32),
            pltpu.VMEM((na, ka, 128), F32),
            pltpu.VMEM((ny, nc, vectors, own), BF16),
            pltpu.VMEM((ny, nc, vectors, own), BF16),
            pltpu.VMEM((vectors, own), F32),
            pltpu.VMEM((nc, 1, 128), F32),
            pltpu.VMEM((npairs * ny, 1, 128), F32),
            pltpu.SemaphoreType.DMA((nx,)),
            pltpu.SemaphoreType.DMA((2,)),
            pltpu.SemaphoreType.DMA((ny, nc)),
            pltpu.SemaphoreType.DMA((10,)),
            pltpu.SemaphoreType.DMA((10,)),
        ],
        compiler_params=pltpu.CompilerParams(
            collective_id=0, has_side_effects=True, vmem_limit_bytes=60 * 1024 * 1024
        ),
        name="sigma_build",
    )(integrals, energy_gaps.reshape(1, rows), trial_vectors.T)
    sigma, subspace, residuals, norms = pl.pallas_call(
        put_out,
        out_shape=tuple(jax.ShapeDtypeStruct(s, F32) for s in shapes),
        in_specs=[vmem] * 4,
        out_specs=(hbm,) * 4,
        scratch_shapes=[pltpu.SemaphoreType.DMA((4,))],
        name="put_out",
    )(*[pltpu.with_memory_space_constraint(r, pltpu.VMEM) for r in results])
    return sigma.T, subspace, residuals.T, norms.reshape(vectors)


def solution(mesh):
    sizes = (8, 4, 4, 2)
    finer = Mesh(mesh.devices.reshape(sizes), AXES)
    return build(finer, sizes)


def build(finer, sizes):
    return jax.shard_map(
        functools.partial(local, sizes),
        mesh=finer,
        in_specs=(P(PAIR, AUX), P(PAIR), P(PAIR, None)),
        out_specs=(P(PAIR + AUX, None), P(), P(PAIR + AUX, None), P()),
        check_vma=False,
    )
```

```python
import functools

import jax
import jax.numpy as jnp
from jax import lax
from jax.experimental import pallas as pl
from jax.experimental.pallas import tpu as pltpu
from jax.sharding import Mesh
from jax.sharding import PartitionSpec as P

AXES = ("z", "x", "y", "c")
PAIR = ("z", "x")
AUX = ("y", "c")
EPSILON = 1e-06
PIECES = 4
F32 = jnp.float32
BF16 = jnp.bfloat16
NT = (((1,), (1,)), ((), ()))


def farthest(n):
    return sorted(range(n), key=lambda d: -min(d, n - d))


def far_first(i, n):
    step = lax.div(i + 1, 2)
    return n // 2 + step * (1 - 2 * lax.rem(i, 2))


def kernel(
    sizes,
    integrals,
    gaps,
    trial,
    sigma,
    subspace,
    residuals,
    norms,
    held,
    turned,
    v,
    g,
    vh,
    parts,
    parts_in,
    half,
    at,
    mx,
    mz,
    gc,
    gy,
    prows,
    terms,
    terms_in,
    chip_out,
    chip_in,
    coupled,
    nchip,
    nall,
    load_sem,
    small_load,
    terms_sem,
    chip_sem,
    send_sem,
    recv_sem,
):
    nz, nx, ny, nc = sizes
    na, npairs = ny * nc, nz * nx
    vectors, rows = v.shape
    columns = held.shape[1]
    kz, cx = vectors // nz, columns // nx
    own, ka = rows // na, vectors // na
    total_pairs = float(rows * npairs)
    z, x, y, c = (lax.axis_index(n) for n in AXES)
    a = y * nc + c
    me = z * nx + x

    zs, xs, ys, cs = ([lax.rem(p + d, n) for d in range(n)] for p, n in zip((z, x, y, c), sizes))
    plane = [(zs[i], xs[j], y, c) for i in farthest(nz) for j in farthest(nx)][:-1]
    group = [(z, x, ys[i], cs[j]) for i in farthest(ny) for j in reversed(range(nc))][:-1]
    sibling = (z, x, y, cs[1])
    y_others = [(z, x, ys[i], c) for i in farthest(ny)][:-1]
    x_others = [(z, xs[j], y, c) for j in farthest(nx)][:-1]
    z_others = [(zs[i], x, y, c) for i in farthest(nz)][:-1]

    def send(src, dst, k, to):
        pltpu.make_async_remote_copy(
            src_ref=src,
            dst_ref=dst,
            send_sem=send_sem.at[k],
            recv_sem=recv_sem.at[k],
            device_id=to,
            device_id_type=pl.DeviceIdType.MESH,
        ).start()

    def arrived(ref, k):
        pltpu.make_async_remote_copy(
            src_ref=ref,
            dst_ref=ref,
            send_sem=send_sem.at[k],
            recv_sem=recv_sem.at[k],
            device_id=sibling,
            device_id_type=pl.DeviceIdType.MESH,
        ).wait_recv()

    def sent(ref, k):
        pltpu.make_async_remote_copy(
            src_ref=ref,
            dst_ref=ref,
            send_sem=send_sem.at[k],
            recv_sem=recv_sem.at[k],
            device_id=sibling,
            device_id_type=pl.DeviceIdType.MESH,
        ).wait_send()

    def each(n, body):
        def step(i, carry):
            body(i)
            return carry

        lax.fori_loop(0, n, step, 0)

    load_v = pltpu.make_async_copy(trial, v, small_load.at[0])
    load_g = pltpu.make_async_copy(gaps, g, small_load.at[1])
    load_v.start()
    load_g.start()

    def columns_of(i):
        xx = lax.rem(x + far_first(i, nx), nx)
        return pl.ds(pl.multiple_of(xx * cx, 128), cx)

    piece = rows // PIECES

    def load_chunk(i):
        for p in range(PIECES):
            where = (pl.ds(p * piece, piece), columns_of(i))
            pltpu.make_async_copy(integrals.at[where], held.at[where], load_sem.at[i]).start()

    load_chunk(0)
    barrier = pltpu.get_barrier_semaphore()
    for to in plane + group:
        pl.semaphore_signal(barrier, inc=1, device_id=to, device_id_type=pl.DeviceIdType.MESH)
    for i in range(1, nx):
        load_chunk(i)

    load_v.wait()
    load_g.wait()
    vh[...] = v[...].astype(BF16)

    def scatter(i):
        xx = lax.rem(x + far_first(i, nx), nx)
        for j, oz in enumerate(farthest(nz)[:-1]):
            send(parts.at[i, zs[oz]], parts_in.at[j * nx + i], 0, (zs[oz], xx, y, c))

        @pl.when(i < nx - 1)
        def _():
            send(parts.at[i, z], parts_in.at[(nz - 1) * nx + i], 0, (z, xx, y, c))

    def first_product(i):
        cols = columns_of(i)
        pltpu.make_async_copy(integrals.at[:, cols], held.at[:, cols], load_sem.at[i]).wait()
        part = jnp.dot(vh[...], held[:, cols], preferred_element_type=F32)
        parts[i] = part.astype(BF16).reshape(nz, kz, cx)

        @pl.when(i == 1)
        def _():
            pl.semaphore_wait(barrier, len(plane) + len(group))
            scatter(0)

        @pl.when(i > 0)
        def _():
            scatter(i)

    each(nx, first_product)

    first = pl.multiple_of(a * ka, ka)
    mine = v[pl.ds(first, ka), :]
    gv = v[...] * g[...]
    m1 = lax.dot_general(mine, gv, NT, precision=lax.Precision.HIGHEST, preferred_element_type=F32)
    squares = jnp.sum(mine * mine, axis=1, keepdims=True)
    mx[x] = jnp.concatenate([m1, jnp.broadcast_to(squares, (ka, vectors))], axis=1)
    for to in x_others:
        send(mx.at[x], mx.at[x], 1, to)

    def turn(i):
        block = pl.ds(pl.multiple_of(i * 128, 128), 128)
        turned[:, block] = held[block, :].T

    each(rows // 256, turn)

    arrived(parts_in, 0)
    block = parts[nx - 1, z].astype(F32)
    block = block + jnp.sum(parts_in[...].astype(F32), axis=0)
    slot = x * nz + z
    half[slot] = block.astype(BF16)
    for to in plane:
        send(half.at[slot], half.at[slot], 2, to)

    arrived(mx.at[pl.ds(0, nx - 1)], 1)
    mz[z] = jnp.sum(mx[...], axis=0)
    for to in z_others:
        send(mz.at[z], mz.at[z], 3, to)

    each(rows // 256, lambda i: turn(rows // 256 + i))

    arrived(mz.at[pl.ds(0, nz - 1)], 3)
    prows[a] = jnp.sum(mz[...], axis=0)
    for to in group:
        send(prows.at[a], prows.at[a], 6, to)

    arrived(half.at[pl.ds(0, npairs - 1)], 2)
    for i in range(nx):
        at[:, i * cx : (i + 1) * cx] = half[i * nz : (i + 1) * nz].reshape(vectors, cx)

    low = vectors // 2
    gram = lax.dot_general(at[...], at[...], NT, preferred_element_type=F32)
    gc[c] = jnp.concatenate([gram[:low], gram[low:]], axis=1)
    send(gc.at[c], gc.at[c], 4, sibling)

    def share_gram():
        arrived(gc.at[0], 4)
        gy[y] = gc[0] + gc[1]
        for to in y_others:
            send(gy.at[y], gy.at[y], 7, to)

    @pl.when(c == 0)
    def _():
        share_gram()

    def pass_on(i):
        pltpu.make_async_remote_copy(
            src_ref=chip_out.at[i],
            dst_ref=chip_in.at[i],
            send_sem=send_sem.at[10],
            recv_sem=chip_sem.at[i],
            device_id=sibling,
            device_id_type=pl.DeviceIdType.MESH,
        ).wait_recv()
        whole = coupled[i] + chip_in[i].astype(F32)

        @pl.when(i < ny - 1)
        def _():
            terms[i] = whole.astype(BF16)
            pltpu.make_async_remote_copy(
                src_ref=terms.at[i],
                dst_ref=terms_in.at[i],
                send_sem=send_sem.at[5],
                recv_sem=terms_sem.at[i],
                device_id=(z, x, lax.rem(y + far_first(i, ny), ny), c),
                device_id_type=pl.DeviceIdType.MESH,
            ).start()

        @pl.when(i == ny - 1)
        def _():
            coupled[i] = whole

    def second_product(i):
        yy = lax.rem(y + far_first(i, ny), ny)
        begin = pl.multiple_of(yy * nc * own, 128)
        out = jnp.dot(at[...], turned[:, pl.ds(begin, nc * own)], preferred_element_type=F32)
        theirs = jnp.where(c == 0, out[:, own:], out[:, :own])
        chip_out[i] = theirs.astype(BF16)
        pltpu.make_async_remote_copy(
            src_ref=chip_out.at[i],
            dst_ref=chip_in.at[i],
            send_sem=send_sem.at[10],
            recv_sem=chip_sem.at[i],
            device_id=sibling,
            device_id_type=pl.DeviceIdType.MESH,
        ).start()
        coupled[i] = jnp.where(c == 0, out[:, :own], out[:, own:])

        @pl.when(c == 0)
        def _():
            pass_on(i)

    each(ny, second_product)

    @pl.when(c > 0)
    def _():
        share_gram()
        each(ny, pass_on)

    mine_at = pl.ds(pl.multiple_of(a * own, 128), own)
    own_trial = v[:, mine_at]

    arrived(prows.at[pl.ds(0, na - 1)], 6)
    arrived(gy.at[pl.ds(0, ny - 1)], 7)
    gram = jnp.sum(gy[...], axis=0)
    gram = jnp.concatenate([gram[:, :vectors], gram[:, vectors:]], axis=0)
    inputs = prows[...].reshape(vectors, 2 * vectors)
    sub = (inputs[:, :vectors] + 2.0 * gram) / total_pairs
    row = lax.broadcasted_iota(jnp.int32, (vectors, vectors), 0)
    lane = lax.broadcasted_iota(jnp.int32, (vectors, vectors), 1)
    diagonal = jnp.sum(jnp.where(row == lane, sub, 0.0), axis=1, keepdims=True)
    intersection = inputs[:, vectors : vectors + 1] / total_pairs
    rayleigh = diagonal / (intersection + EPSILON)
    subspace[...] = sub

    total = coupled[ny - 1]
    for i in range(ny - 1):
        pltpu.make_async_remote_copy(
            src_ref=terms.at[i],
            dst_ref=terms_in.at[i],
            send_sem=send_sem.at[5],
            recv_sem=terms_sem.at[i],
            device_id=sibling,
            device_id_type=pl.DeviceIdType.MESH,
        ).wait_recv()
        total = total + terms_in[i].astype(F32)

    sigma_own = own_trial * g[:, mine_at] + 2.0 * total
    sigma[...] = sigma_own
    residual = sigma_own - rayleigh * own_trial
    residuals[...] = residual
    squared = residual * residual
    lanes = squared[:, :128]
    for i in range(1, own // 128):
        lanes = lanes + squared[:, i * 128 : (i + 1) * 128]
    lanes = jnp.concatenate([lanes, jnp.zeros((128 - vectors, 128), F32)], axis=0)
    nchip[c] = jnp.sum(lanes.T, axis=0, keepdims=True)
    send(nchip.at[c], nchip.at[c], 8, sibling)

    arrived(nchip.at[0], 8)
    nall[me * ny + y] = nchip[0] + nchip[1]

    def share(t):
        zz = lax.rem(z + far_first(t, nz), nz)
        spots = [(zz, xs[j], ys[k], c) for j in farthest(nx) for k in farthest(ny)]
        for to in spots[:-1]:
            send(nall.at[me * ny + y], nall.at[me * ny + y], 9, to)

        @pl.when(t < nz - 1)
        def _():
            send(nall.at[me * ny + y], nall.at[me * ny + y], 9, spots[-1])

    each(nz, share)

    sent(parts_in, 0)
    sent(mx.at[pl.ds(0, nx - 1)], 1)
    sent(half.at[pl.ds(0, npairs - 1)], 2)
    sent(mz.at[pl.ds(0, nz - 1)], 3)
    sent(gc.at[0], 4)
    sent(terms, 5)
    sent(chip_out, 10)
    sent(prows.at[pl.ds(0, na - 1)], 6)
    sent(gy.at[pl.ds(0, ny - 1)], 7)
    sent(nchip.at[0], 8)

    arrived(nall.at[pl.ds(0, npairs * ny - 1)], 9)
    sent(nall.at[pl.ds(0, npairs * ny - 1)], 9)
    total = jnp.sum(nall[...], axis=0) / total_pairs
    norms[...] = jnp.sqrt(total[:, :vectors] + EPSILON)


def put_out(*refs):
    copies = [pltpu.make_async_copy(refs[i], refs[4 + i], refs[8].at[i]) for i in range(4)]
    for copy in copies:
        copy.start()
    for copy in copies:
        copy.wait()


def local(sizes, integrals, energy_gaps, trial_vectors):
    nz, nx, ny, nc = sizes
    na, npairs = ny * nc, nz * nx
    rows, columns = integrals.shape
    vectors = trial_vectors.shape[1]
    kz, cx = vectors // nz, columns // nx
    own, ka = rows // na, vectors // na
    hbm = pl.BlockSpec(memory_space=pl.ANY)
    vmem = pl.BlockSpec(memory_space=pltpu.VMEM)
    shapes = ((vectors, own), (vectors, vectors), (vectors, own), (1, vectors))
    results = pl.pallas_call(
        functools.partial(kernel, sizes),
        out_shape=tuple(pltpu.VMEM(s, F32) for s in shapes),
        in_specs=[hbm, hbm, hbm],
        out_specs=(vmem,) * 4,
        scratch_shapes=[
            pltpu.VMEM((rows, columns), BF16),
            pltpu.VMEM((columns, rows), BF16),
            pltpu.VMEM((vectors, rows), F32),
            pltpu.VMEM((1, rows), F32),
            pltpu.VMEM((vectors, rows), BF16),
            pltpu.VMEM((nx, nz, kz, cx), BF16),
            pltpu.VMEM((npairs - 1, kz, cx), BF16),
            pltpu.VMEM((npairs, kz, cx), BF16),
            pltpu.VMEM((vectors, columns), BF16),
            pltpu.VMEM((nx, ka, 128), F32),
            pltpu.VMEM((nz, ka, 128), F32),
            pltpu.VMEM((nc, vectors // 2, 2 * vectors), F32),
            pltpu.VMEM((ny, vectors // 2, 2 * vectors), F32),
            pltpu.VMEM((na, ka, 128), F32),
            pltpu.VMEM((ny - 1, vectors, own), BF16),
            pltpu.VMEM((ny - 1, vectors, own), BF16),
            pltpu.VMEM((ny, vectors, own), BF16),
            pltpu.VMEM((ny, vectors, own), BF16),
            pltpu.VMEM((ny, vectors, own), F32),
            pltpu.VMEM((nc, 1, 128), F32),
            pltpu.VMEM((npairs * ny, 1, 128), F32),
            pltpu.SemaphoreType.DMA((nx,)),
            pltpu.SemaphoreType.DMA((2,)),
            pltpu.SemaphoreType.DMA((ny - 1,)),
            pltpu.SemaphoreType.DMA((ny,)),
            pltpu.SemaphoreType.DMA((11,)),
            pltpu.SemaphoreType.DMA((11,)),
        ],
        compiler_params=pltpu.CompilerParams(
            collective_id=0, has_side_effects=True, vmem_limit_bytes=60 * 1024 * 1024
        ),
        name="sigma_build",
    )(integrals, energy_gaps.reshape(1, rows), trial_vectors.T)
    sigma, subspace, residuals, norms = pl.pallas_call(
        put_out,
        out_shape=tuple(jax.ShapeDtypeStruct(s, F32) for s in shapes),
        in_specs=[vmem] * 4,
        out_specs=(hbm,) * 4,
        scratch_shapes=[pltpu.SemaphoreType.DMA((4,))],
        name="put_out",
    )(*[pltpu.with_memory_space_constraint(r, pltpu.VMEM) for r in results])
    return sigma.T, subspace, residuals.T, norms.reshape(vectors)


def solution(mesh):
    sizes = (8, 4, 4, 2)
    finer = Mesh(mesh.devices.reshape(sizes), AXES)
    return build(finer, sizes)


def build(finer, sizes):
    return jax.shard_map(
        functools.partial(local, sizes),
        mesh=finer,
        in_specs=(P(PAIR, AUX), P(PAIR), P(PAIR, None)),
        out_specs=(P(PAIR + AUX, None), P(), P(PAIR + AUX, None), P()),
        check_vma=False,
    )
```

```python
import functools

import jax
import jax.numpy as jnp
from jax import lax
from jax.experimental import pallas as pl
from jax.experimental.pallas import tpu as pltpu
from jax.sharding import Mesh
from jax.sharding import PartitionSpec as P

AXES = ("z", "x", "y", "c")
PAIR = ("z", "x")
AUX = ("y", "c")
EPSILON = 1e-06
PIECES = 4
HALVES = 2
F32 = jnp.float32
BF16 = jnp.bfloat16
NT = (((1,), (1,)), ((), ()))


def farthest(n):
    return sorted(range(n), key=lambda d: -min(d, n - d))


def far_first(i, n):
    step = lax.div(i + 1, 2)
    return n // 2 + step * (1 - 2 * lax.rem(i, 2))


def kernel(
    sizes,
    integrals,
    gaps,
    trial,
    sigma,
    subspace,
    residuals,
    norms,
    held,
    turned,
    v,
    g,
    vh,
    parts,
    parts_in,
    half,
    at,
    mx,
    mz,
    gc,
    gy,
    prows,
    terms,
    terms_in,
    chip_out,
    chip_in,
    coupled,
    nchip,
    nall,
    load_sem,
    small_load,
    terms_sem,
    chip_sem,
    send_sem,
    recv_sem,
):
    nz, nx, ny, nc = sizes
    na, npairs = ny * nc, nz * nx
    vectors, rows = v.shape
    columns = held.shape[1]
    kz, cx = vectors // nz, columns // nx
    own, ka = rows // na, vectors // na
    total_pairs = float(rows * npairs)
    z, x, y, c = (lax.axis_index(n) for n in AXES)
    a = y * nc + c
    me = z * nx + x

    zs, xs, ys, cs = ([lax.rem(p + d, n) for d in range(n)] for p, n in zip((z, x, y, c), sizes))
    plane = [(zs[i], xs[j], y, c) for i in farthest(nz) for j in farthest(nx)][:-1]
    group = [(z, x, ys[i], cs[j]) for i in farthest(ny) for j in reversed(range(nc))][:-1]
    sibling = (z, x, y, cs[1])
    y_others = [(z, x, ys[i], c) for i in farthest(ny)][:-1]
    x_others = [(z, xs[j], y, c) for j in farthest(nx)][:-1]
    z_others = [(zs[i], x, y, c) for i in farthest(nz)][:-1]

    def send(src, dst, k, to):
        pltpu.make_async_remote_copy(
            src_ref=src,
            dst_ref=dst,
            send_sem=send_sem.at[k],
            recv_sem=recv_sem.at[k],
            device_id=to,
            device_id_type=pl.DeviceIdType.MESH,
        ).start()

    def arrived(ref, k):
        pltpu.make_async_remote_copy(
            src_ref=ref,
            dst_ref=ref,
            send_sem=send_sem.at[k],
            recv_sem=recv_sem.at[k],
            device_id=sibling,
            device_id_type=pl.DeviceIdType.MESH,
        ).wait_recv()

    def sent(ref, k):
        pltpu.make_async_remote_copy(
            src_ref=ref,
            dst_ref=ref,
            send_sem=send_sem.at[k],
            recv_sem=recv_sem.at[k],
            device_id=sibling,
            device_id_type=pl.DeviceIdType.MESH,
        ).wait_send()

    def each(n, body):
        def step(i, carry):
            body(i)
            return carry

        lax.fori_loop(0, n, step, 0)

    load_v = pltpu.make_async_copy(trial, v, small_load.at[0])
    load_g = pltpu.make_async_copy(gaps, g, small_load.at[1])
    load_v.start()
    load_g.start()

    def columns_of(i):
        xx = lax.rem(x + far_first(i, nx), nx)
        return pl.ds(pl.multiple_of(xx * cx, 128), cx)

    piece = rows // PIECES

    def load_chunk(i):
        for p in range(PIECES):
            where = (pl.ds(p * piece, piece), columns_of(i))
            sem = load_sem.at[i, p * HALVES // PIECES]
            pltpu.make_async_copy(integrals.at[where], held.at[where], sem).start()

    load_chunk(0)
    barrier = pltpu.get_barrier_semaphore()
    for to in plane + group:
        pl.semaphore_signal(barrier, inc=1, device_id=to, device_id_type=pl.DeviceIdType.MESH)
    for i in range(1, nx):
        load_chunk(i)

    load_v.wait()
    load_g.wait()
    vh[...] = v[...].astype(BF16)

    def scatter(i):
        xx = lax.rem(x + far_first(i, nx), nx)
        for j, oz in enumerate(farthest(nz)[:-1]):
            send(parts.at[i, zs[oz]], parts_in.at[j * nx + i], 0, (zs[oz], xx, y, c))

        @pl.when(i < nx - 1)
        def _():
            send(parts.at[i, z], parts_in.at[(nz - 1) * nx + i], 0, (z, xx, y, c))

    def first_product(i):
        cols = columns_of(i)
        part = 0.0
        for h in range(HALVES):
            span = pl.ds(h * rows // HALVES, rows // HALVES)
            where = (span, cols)
            pltpu.make_async_copy(integrals.at[where], held.at[where], load_sem.at[i, h]).wait()
            part = part + jnp.dot(vh[:, span], held[where], preferred_element_type=F32)
        parts[i] = part.astype(BF16).reshape(nz, kz, cx)

        @pl.when(i == 1)
        def _():
            pl.semaphore_wait(barrier, len(plane) + len(group))
            scatter(0)

        @pl.when(i > 0)
        def _():
            scatter(i)

    each(nx, first_product)

    first = pl.multiple_of(a * ka, ka)
    mine = v[pl.ds(first, ka), :]
    gv = v[...] * g[...]
    m1 = lax.dot_general(mine, gv, NT, precision=lax.Precision.HIGHEST, preferred_element_type=F32)
    squares = jnp.sum(mine * mine, axis=1, keepdims=True)
    mx[x] = jnp.concatenate([m1, jnp.broadcast_to(squares, (ka, vectors))], axis=1)
    for to in x_others:
        send(mx.at[x], mx.at[x], 1, to)

    def turn(i):
        block = pl.ds(pl.multiple_of(i * 128, 128), 128)
        turned[:, block] = held[block, :].T

    each(rows // 256, turn)

    arrived(mx.at[pl.ds(0, nx - 1)], 1)
    mz[z] = jnp.sum(mx[...], axis=0)
    for to in z_others:
        send(mz.at[z], mz.at[z], 3, to)

    arrived(parts_in, 0)
    block = parts[nx - 1, z].astype(F32)
    block = block + jnp.sum(parts_in[...].astype(F32), axis=0)
    slot = x * nz + z
    half[slot] = block.astype(BF16)
    for to in plane:
        send(half.at[slot], half.at[slot], 2, to)

    each(rows // 256, lambda i: turn(rows // 256 + i))

    arrived(mz.at[pl.ds(0, nz - 1)], 3)
    prows[a] = jnp.sum(mz[...], axis=0)
    for to in group:
        send(prows.at[a], prows.at[a], 6, to)

    arrived(half.at[pl.ds(0, npairs - 1)], 2)
    for i in range(nx):
        at[:, i * cx : (i + 1) * cx] = half[i * nz : (i + 1) * nz].reshape(vectors, cx)

    low = vectors // 2

    def make_gram():
        gram = lax.dot_general(at[...], at[...], NT, preferred_element_type=F32)
        gc[c] = jnp.concatenate([gram[:low], gram[low:]], axis=1)
        send(gc.at[c], gc.at[c], 4, sibling)

    def share_gram():
        arrived(gc.at[0], 4)
        gy[y] = gc[0] + gc[1]
        for to in y_others:
            send(gy.at[y], gy.at[y], 7, to)

    def pass_on(i):
        pltpu.make_async_remote_copy(
            src_ref=chip_out.at[i],
            dst_ref=chip_in.at[i],
            send_sem=send_sem.at[10],
            recv_sem=chip_sem.at[i],
            device_id=sibling,
            device_id_type=pl.DeviceIdType.MESH,
        ).wait_recv()
        whole = coupled[i] + chip_in[i].astype(F32)

        @pl.when(i < ny - 1)
        def _():
            terms[i] = whole.astype(BF16)
            pltpu.make_async_remote_copy(
                src_ref=terms.at[i],
                dst_ref=terms_in.at[i],
                send_sem=send_sem.at[5],
                recv_sem=terms_sem.at[i],
                device_id=(z, x, lax.rem(y + far_first(i, ny), ny), c),
                device_id_type=pl.DeviceIdType.MESH,
            ).start()

        @pl.when(i == ny - 1)
        def _():
            coupled[i] = whole

    def second_product(i):
        yy = lax.rem(y + far_first(i, ny), ny)
        begin = pl.multiple_of(yy * nc * own, 128)
        out = jnp.dot(at[...], turned[:, pl.ds(begin, nc * own)], preferred_element_type=F32)
        kept = c
        chip_out[i] = jnp.where(kept == 0, out[:, own:], out[:, :own]).astype(BF16)
        pltpu.make_async_remote_copy(
            src_ref=chip_out.at[i],
            dst_ref=chip_in.at[i],
            send_sem=send_sem.at[10],
            recv_sem=chip_sem.at[i],
            device_id=sibling,
            device_id_type=pl.DeviceIdType.MESH,
        ).start()
        coupled[i] = jnp.where(kept == 0, out[:, :own], out[:, own:])

        @pl.when(c == 0)
        def _():
            pass_on(i)

        @pl.when(i == 0)
        def _():
            make_gram()

            @pl.when(c == 0)
            def _():
                share_gram()

    each(ny, second_product)

    @pl.when(c > 0)
    def _():
        pass_on(0)
        share_gram()
        each(ny - 1, lambda i: pass_on(i + 1))

    mine_at = pl.ds(pl.multiple_of(a * own, 128), own)
    own_trial = v[:, mine_at]

    arrived(prows.at[pl.ds(0, na - 1)], 6)
    arrived(gy.at[pl.ds(0, ny - 1)], 7)
    gram = jnp.sum(gy[...], axis=0)
    gram = jnp.concatenate([gram[:, :vectors], gram[:, vectors:]], axis=0)
    inputs = prows[...].reshape(vectors, 2 * vectors)
    sub = (inputs[:, :vectors] + 2.0 * gram) / total_pairs
    row = lax.broadcasted_iota(jnp.int32, (vectors, vectors), 0)
    lane = lax.broadcasted_iota(jnp.int32, (vectors, vectors), 1)
    diagonal = jnp.sum(jnp.where(row == lane, sub, 0.0), axis=1, keepdims=True)
    intersection = inputs[:, vectors : vectors + 1] / total_pairs
    rayleigh = diagonal / (intersection + EPSILON)
    subspace[...] = sub

    total = coupled[ny - 1]
    for i in range(ny - 1):
        pltpu.make_async_remote_copy(
            src_ref=terms.at[i],
            dst_ref=terms_in.at[i],
            send_sem=send_sem.at[5],
            recv_sem=terms_sem.at[i],
            device_id=sibling,
            device_id_type=pl.DeviceIdType.MESH,
        ).wait_recv()
        total = total + terms_in[i].astype(F32)

    sigma_own = own_trial * g[:, mine_at] + 2.0 * total
    sigma[...] = sigma_own
    residual = sigma_own - rayleigh * own_trial
    residuals[...] = residual
    squared = residual * residual
    lanes = squared[:, :128]
    for i in range(1, own // 128):
        lanes = lanes + squared[:, i * 128 : (i + 1) * 128]
    lanes = jnp.concatenate([lanes, jnp.zeros((128 - vectors, 128), F32)], axis=0)
    nchip[c] = jnp.sum(lanes.T, axis=0, keepdims=True)
    send(nchip.at[c], nchip.at[c], 8, sibling)

    arrived(nchip.at[0], 8)
    nall[me * ny + y] = nchip[0] + nchip[1]

    def share(t):
        zz = lax.rem(z + far_first(t, nz), nz)
        spots = [(zz, xs[j], ys[k], c) for j in farthest(nx) for k in farthest(ny)]
        for to in spots[:-1]:
            send(nall.at[me * ny + y], nall.at[me * ny + y], 9, to)

        @pl.when(t < nz - 1)
        def _():
            send(nall.at[me * ny + y], nall.at[me * ny + y], 9, spots[-1])

    each(nz, share)

    sent(parts_in, 0)
    sent(mx.at[pl.ds(0, nx - 1)], 1)
    sent(half.at[pl.ds(0, npairs - 1)], 2)
    sent(mz.at[pl.ds(0, nz - 1)], 3)
    sent(gc.at[0], 4)
    sent(terms, 5)
    sent(chip_out, 10)
    sent(prows.at[pl.ds(0, na - 1)], 6)
    sent(gy.at[pl.ds(0, ny - 1)], 7)
    sent(nchip.at[0], 8)

    arrived(nall.at[pl.ds(0, npairs * ny - 1)], 9)
    sent(nall.at[pl.ds(0, npairs * ny - 1)], 9)
    total = jnp.sum(nall[...], axis=0) / total_pairs
    norms[...] = jnp.sqrt(total[:, :vectors] + EPSILON)


def put_out(*refs):
    copies = [pltpu.make_async_copy(refs[i], refs[4 + i], refs[8].at[i]) for i in range(4)]
    for copy in copies:
        copy.start()
    for copy in copies:
        copy.wait()


def local(sizes, integrals, energy_gaps, trial_vectors):
    nz, nx, ny, nc = sizes
    na, npairs = ny * nc, nz * nx
    rows, columns = integrals.shape
    vectors = trial_vectors.shape[1]
    kz, cx = vectors // nz, columns // nx
    own, ka = rows // na, vectors // na
    hbm = pl.BlockSpec(memory_space=pl.ANY)
    vmem = pl.BlockSpec(memory_space=pltpu.VMEM)
    shapes = ((vectors, own), (vectors, vectors), (vectors, own), (1, vectors))
    results = pl.pallas_call(
        functools.partial(kernel, sizes),
        out_shape=tuple(pltpu.VMEM(s, F32) for s in shapes),
        in_specs=[hbm, hbm, hbm],
        out_specs=(vmem,) * 4,
        scratch_shapes=[
            pltpu.VMEM((rows, columns), BF16),
            pltpu.VMEM((columns, rows), BF16),
            pltpu.VMEM((vectors, rows), F32),
            pltpu.VMEM((1, rows), F32),
            pltpu.VMEM((vectors, rows), BF16),
            pltpu.VMEM((nx, nz, kz, cx), BF16),
            pltpu.VMEM((npairs - 1, kz, cx), BF16),
            pltpu.VMEM((npairs, kz, cx), BF16),
            pltpu.VMEM((vectors, columns), BF16),
            pltpu.VMEM((nx, ka, 128), F32),
            pltpu.VMEM((nz, ka, 128), F32),
            pltpu.VMEM((nc, vectors // 2, 2 * vectors), F32),
            pltpu.VMEM((ny, vectors // 2, 2 * vectors), F32),
            pltpu.VMEM((na, ka, 128), F32),
            pltpu.VMEM((ny - 1, vectors, own), BF16),
            pltpu.VMEM((ny - 1, vectors, own), BF16),
            pltpu.VMEM((ny, vectors, own), BF16),
            pltpu.VMEM((ny, vectors, own), BF16),
            pltpu.VMEM((ny, vectors, own), F32),
            pltpu.VMEM((nc, 1, 128), F32),
            pltpu.VMEM((npairs * ny, 1, 128), F32),
            pltpu.SemaphoreType.DMA((nx, HALVES)),
            pltpu.SemaphoreType.DMA((2,)),
            pltpu.SemaphoreType.DMA((ny - 1,)),
            pltpu.SemaphoreType.DMA((ny,)),
            pltpu.SemaphoreType.DMA((11,)),
            pltpu.SemaphoreType.DMA((11,)),
        ],
        compiler_params=pltpu.CompilerParams(
            collective_id=0, has_side_effects=True, vmem_limit_bytes=60 * 1024 * 1024
        ),
        name="sigma_build",
    )(integrals, energy_gaps.reshape(1, rows), trial_vectors.T)
    sigma, subspace, residuals, norms = pl.pallas_call(
        put_out,
        out_shape=tuple(jax.ShapeDtypeStruct(s, F32) for s in shapes),
        in_specs=[vmem] * 4,
        out_specs=(hbm,) * 4,
        scratch_shapes=[pltpu.SemaphoreType.DMA((4,))],
        name="put_out",
    )(*[pltpu.with_memory_space_constraint(r, pltpu.VMEM) for r in results])
    return sigma.T, subspace, residuals.T, norms.reshape(vectors)


def solution(mesh):
    sizes = (8, 4, 4, 2)
    finer = Mesh(mesh.devices.reshape(sizes), AXES)
    return build(finer, sizes)


def build(finer, sizes):
    return jax.shard_map(
        functools.partial(local, sizes),
        mesh=finer,
        in_specs=(P(PAIR, AUX), P(PAIR), P(PAIR, None)),
        out_specs=(P(PAIR + AUX, None), P(), P(PAIR + AUX, None), P()),
        check_vma=False,
    )
```

```python
import functools

import jax
import jax.numpy as jnp
from jax import lax
from jax.experimental import pallas as pl
from jax.experimental.pallas import tpu as pltpu
from jax.sharding import Mesh
from jax.sharding import PartitionSpec as P

AXES = ("z", "x", "y", "c")
PAIR = ("z", "x")
AUX = ("y", "c")
EPSILON = 1e-06
PIECES = 4
HALVES = 2
F32 = jnp.float32
BF16 = jnp.bfloat16
NT = (((1,), (1,)), ((), ()))


def farthest(n):
    return sorted(range(n), key=lambda d: -min(d, n - d))


def far_first(i, n):
    step = lax.div(i + 1, 2)
    return n // 2 + step * (1 - 2 * lax.rem(i, 2))


def kernel(
    sizes,
    integrals,
    gaps,
    trial,
    sigma,
    subspace,
    residuals,
    norms,
    held,
    turned,
    v,
    g,
    vh,
    parts,
    parts_in,
    half,
    at,
    mx,
    mz,
    gc,
    gy,
    prows,
    terms,
    terms_in,
    chip_out,
    chip_in,
    coupled,
    nchip,
    nall,
    load_sem,
    small_load,
    terms_sem,
    chip_sem,
    send_sem,
    recv_sem,
):
    nz, nx, ny, nc = sizes
    na, npairs = ny * nc, nz * nx
    vectors, rows = v.shape
    columns = held.shape[1]
    kz, cx = vectors // nz, columns // nx
    own, ka = rows // na, vectors // na
    total_pairs = float(rows * npairs)
    z, x, y, c = (lax.axis_index(n) for n in AXES)
    a = y * nc + c
    me = z * nx + x

    zs, xs, ys, cs = ([lax.rem(p + d, n) for d in range(n)] for p, n in zip((z, x, y, c), sizes))
    plane = [(zs[i], xs[j], y, c) for i in farthest(nz) for j in farthest(nx)][:-1]
    group = [(z, x, ys[i], cs[j]) for i in farthest(ny) for j in reversed(range(nc))][:-1]
    sibling = (z, x, y, cs[1])
    y_others = [(z, x, ys[i], c) for i in farthest(ny)][:-1]
    x_others = [(z, xs[j], y, c) for j in farthest(nx)][:-1]
    z_others = [(zs[i], x, y, c) for i in farthest(nz)][:-1]

    def send(src, dst, k, to):
        pltpu.make_async_remote_copy(
            src_ref=src,
            dst_ref=dst,
            send_sem=send_sem.at[k],
            recv_sem=recv_sem.at[k],
            device_id=to,
            device_id_type=pl.DeviceIdType.MESH,
        ).start()

    def arrived(ref, k):
        pltpu.make_async_remote_copy(
            src_ref=ref,
            dst_ref=ref,
            send_sem=send_sem.at[k],
            recv_sem=recv_sem.at[k],
            device_id=sibling,
            device_id_type=pl.DeviceIdType.MESH,
        ).wait_recv()

    def sent(ref, k):
        pltpu.make_async_remote_copy(
            src_ref=ref,
            dst_ref=ref,
            send_sem=send_sem.at[k],
            recv_sem=recv_sem.at[k],
            device_id=sibling,
            device_id_type=pl.DeviceIdType.MESH,
        ).wait_send()

    def each(n, body):
        def step(i, carry):
            body(i)
            return carry

        lax.fori_loop(0, n, step, 0)

    load_v = pltpu.make_async_copy(trial, v, small_load.at[0])
    load_g = pltpu.make_async_copy(gaps, g, small_load.at[1])
    load_v.start()
    load_g.start()

    def columns_of(i):
        xx = lax.rem(x + far_first(i, nx), nx)
        return pl.ds(pl.multiple_of(xx * cx, 128), cx)

    piece = rows // PIECES

    def load_chunk(i):
        for p in range(PIECES):
            where = (pl.ds(p * piece, piece), columns_of(i))
            sem = load_sem.at[i, p * HALVES // PIECES]
            pltpu.make_async_copy(integrals.at[where], held.at[where], sem).start()

    load_chunk(0)
    barrier = pltpu.get_barrier_semaphore()
    for to in plane + group:
        pl.semaphore_signal(barrier, inc=1, device_id=to, device_id_type=pl.DeviceIdType.MESH)
    for i in range(1, nx):
        load_chunk(i)

    load_v.wait()
    load_g.wait()
    vh[...] = v[...].astype(BF16)

    def scatter(i):
        xx = lax.rem(x + far_first(i, nx), nx)
        for j, oz in enumerate(farthest(nz)[:-1]):
            send(parts.at[i, zs[oz]], parts_in.at[j * nx + i], 0, (zs[oz], xx, y, c))

        @pl.when(i < nx - 1)
        def _():
            send(parts.at[i, z], parts_in.at[(nz - 1) * nx + i], 0, (z, xx, y, c))

    def first_product(i):
        cols = columns_of(i)
        part = 0.0
        for h in range(HALVES):
            span = pl.ds(h * rows // HALVES, rows // HALVES)
            where = (span, cols)
            pltpu.make_async_copy(integrals.at[where], held.at[where], load_sem.at[i, h]).wait()
            part = part + jnp.dot(vh[:, span], held[where], preferred_element_type=F32)
        parts[i] = part.astype(BF16).reshape(nz, kz, cx)

        @pl.when(i == 1)
        def _():
            pl.semaphore_wait(barrier, len(plane) + len(group))
            scatter(0)

        @pl.when(i > 0)
        def _():
            scatter(i)

    each(nx, first_product)

    first = pl.multiple_of(a * ka, ka)
    mine = v[pl.ds(first, ka), :]
    gv = v[...] * g[...]
    m1 = lax.dot_general(mine, gv, NT, precision=lax.Precision.HIGHEST, preferred_element_type=F32)
    squares = jnp.sum(mine * mine, axis=1, keepdims=True)
    mx[x] = jnp.concatenate([m1, jnp.broadcast_to(squares, (ka, vectors))], axis=1)
    for to in x_others:
        send(mx.at[x], mx.at[x], 1, to)

    def turn(i):
        block = pl.ds(pl.multiple_of(i * 128, 128), 128)
        turned[:, block] = held[block, :].T

    each(rows // 256, turn)

    arrived(mx.at[pl.ds(0, nx - 1)], 1)
    mz[z] = jnp.sum(mx[...], axis=0)
    for to in z_others:
        send(mz.at[z], mz.at[z], 3, to)

    arrived(parts_in, 0)
    block = parts[nx - 1, z].astype(F32)
    block = block + jnp.sum(parts_in[...].astype(F32), axis=0)
    slot = x * nz + z
    half[slot] = block.astype(BF16)
    for to in plane:
        send(half.at[slot], half.at[slot], 2, to)

    each(rows // 256, lambda i: turn(rows // 256 + i))

    arrived(mz.at[pl.ds(0, nz - 1)], 3)
    prows[a] = jnp.sum(mz[...], axis=0)
    for to in group:
        send(prows.at[a], prows.at[a], 6, to)

    arrived(half.at[pl.ds(0, npairs - 1)], 2)
    for i in range(nx):
        at[:, i * cx : (i + 1) * cx] = half[i * nz : (i + 1) * nz].reshape(vectors, cx)

    low = vectors // 2
    gram = lax.dot_general(at[...], at[...], NT, preferred_element_type=F32)
    gc[c] = jnp.concatenate([gram[:low], gram[low:]], axis=1)
    send(gc.at[c], gc.at[c], 4, sibling)

    def share_gram():
        arrived(gc.at[0], 4)
        gy[y] = gc[0] + gc[1]
        for to in y_others:
            send(gy.at[y], gy.at[y], 7, to)

    @pl.when(c == 0)
    def _():
        share_gram()

    def pass_on(i):
        pltpu.make_async_remote_copy(
            src_ref=chip_out.at[i],
            dst_ref=chip_in.at[i],
            send_sem=send_sem.at[10],
            recv_sem=chip_sem.at[i],
            device_id=sibling,
            device_id_type=pl.DeviceIdType.MESH,
        ).wait_recv()
        whole = coupled[i] + chip_in[i].astype(F32)

        @pl.when(i < ny - 1)
        def _():
            terms[i] = whole.astype(BF16)
            pltpu.make_async_remote_copy(
                src_ref=terms.at[i],
                dst_ref=terms_in.at[i],
                send_sem=send_sem.at[5],
                recv_sem=terms_sem.at[i],
                device_id=(z, x, lax.rem(y + far_first(i, ny), ny), c),
                device_id_type=pl.DeviceIdType.MESH,
            ).start()

        @pl.when(i == ny - 1)
        def _():
            coupled[i] = whole

    def second_product(i):
        yy = lax.rem(y + far_first(i, ny), ny)
        begin = pl.multiple_of(yy * nc * own, 128)
        out = jnp.dot(at[...], turned[:, pl.ds(begin, nc * own)], preferred_element_type=F32)
        theirs = jnp.where(c == 0, out[:, own:], out[:, :own])
        chip_out[i] = theirs.astype(BF16)
        pltpu.make_async_remote_copy(
            src_ref=chip_out.at[i],
            dst_ref=chip_in.at[i],
            send_sem=send_sem.at[10],
            recv_sem=chip_sem.at[i],
            device_id=sibling,
            device_id_type=pl.DeviceIdType.MESH,
        ).start()
        coupled[i] = jnp.where(c == 0, out[:, :own], out[:, own:])

        @pl.when(c == 0)
        def _():
            pass_on(i)

    each(ny, second_product)

    @pl.when(c > 0)
    def _():
        share_gram()
        each(ny, pass_on)

    mine_at = pl.ds(pl.multiple_of(a * own, 128), own)
    own_trial = v[:, mine_at]

    arrived(prows.at[pl.ds(0, na - 1)], 6)
    arrived(gy.at[pl.ds(0, ny - 1)], 7)
    gram = jnp.sum(gy[...], axis=0)
    gram = jnp.concatenate([gram[:, :vectors], gram[:, vectors:]], axis=0)
    inputs = prows[...].reshape(vectors, 2 * vectors)
    sub = (inputs[:, :vectors] + 2.0 * gram) / total_pairs
    row = lax.broadcasted_iota(jnp.int32, (vectors, vectors), 0)
    lane = lax.broadcasted_iota(jnp.int32, (vectors, vectors), 1)
    diagonal = jnp.sum(jnp.where(row == lane, sub, 0.0), axis=1, keepdims=True)
    intersection = inputs[:, vectors : vectors + 1] / total_pairs
    rayleigh = diagonal / (intersection + EPSILON)
    subspace[...] = sub

    total = coupled[ny - 1]
    for i in range(ny - 1):
        pltpu.make_async_remote_copy(
            src_ref=terms.at[i],
            dst_ref=terms_in.at[i],
            send_sem=send_sem.at[5],
            recv_sem=terms_sem.at[i],
            device_id=sibling,
            device_id_type=pl.DeviceIdType.MESH,
        ).wait_recv()
        total = total + terms_in[i].astype(F32)

    sigma_own = own_trial * g[:, mine_at] + 2.0 * total
    sigma[...] = sigma_own
    residual = sigma_own - rayleigh * own_trial
    residuals[...] = residual
    squared = residual * residual
    lanes = squared[:, :128]
    for i in range(1, own // 128):
        lanes = lanes + squared[:, i * 128 : (i + 1) * 128]
    lanes = jnp.concatenate([lanes, jnp.zeros((128 - vectors, 128), F32)], axis=0)
    nchip[c] = jnp.sum(lanes.T, axis=0, keepdims=True)
    send(nchip.at[c], nchip.at[c], 8, sibling)

    arrived(nchip.at[0], 8)
    nall[me * ny + y] = nchip[0] + nchip[1]

    def share(t):
        zz = lax.rem(z + far_first(t, nz), nz)
        spots = [(zz, xs[j], ys[k], c) for j in farthest(nx) for k in farthest(ny)]
        for to in spots[:-1]:
            send(nall.at[me * ny + y], nall.at[me * ny + y], 9, to)

        @pl.when(t < nz - 1)
        def _():
            send(nall.at[me * ny + y], nall.at[me * ny + y], 9, spots[-1])

    each(nz, share)

    sent(parts_in, 0)
    sent(mx.at[pl.ds(0, nx - 1)], 1)
    sent(half.at[pl.ds(0, npairs - 1)], 2)
    sent(mz.at[pl.ds(0, nz - 1)], 3)
    sent(gc.at[0], 4)
    sent(terms, 5)
    sent(chip_out, 10)
    sent(prows.at[pl.ds(0, na - 1)], 6)
    sent(gy.at[pl.ds(0, ny - 1)], 7)
    sent(nchip.at[0], 8)

    arrived(nall.at[pl.ds(0, npairs * ny - 1)], 9)
    sent(nall.at[pl.ds(0, npairs * ny - 1)], 9)
    total = jnp.sum(nall[...], axis=0) / total_pairs
    norms[...] = jnp.sqrt(total[:, :vectors] + EPSILON)


def put_out(*refs):
    copies = [pltpu.make_async_copy(refs[i], refs[4 + i], refs[8].at[i]) for i in range(4)]
    for copy in copies:
        copy.start()
    for copy in copies:
        copy.wait()


def local(sizes, integrals, energy_gaps, trial_vectors):
    nz, nx, ny, nc = sizes
    na, npairs = ny * nc, nz * nx
    rows, columns = integrals.shape
    vectors = trial_vectors.shape[1]
    kz, cx = vectors // nz, columns // nx
    own, ka = rows // na, vectors // na
    hbm = pl.BlockSpec(memory_space=pl.ANY)
    vmem = pl.BlockSpec(memory_space=pltpu.VMEM)
    shapes = ((vectors, own), (vectors, vectors), (vectors, own), (1, vectors))
    results = pl.pallas_call(
        functools.partial(kernel, sizes),
        out_shape=tuple(pltpu.VMEM(s, F32) for s in shapes),
        in_specs=[hbm, hbm, hbm],
        out_specs=(vmem,) * 4,
        scratch_shapes=[
            pltpu.VMEM((rows, columns), BF16),
            pltpu.VMEM((columns, rows), BF16),
            pltpu.VMEM((vectors, rows), F32),
            pltpu.VMEM((1, rows), F32),
            pltpu.VMEM((vectors, rows), BF16),
            pltpu.VMEM((nx, nz, kz, cx), BF16),
            pltpu.VMEM((npairs - 1, kz, cx), BF16),
            pltpu.VMEM((npairs, kz, cx), BF16),
            pltpu.VMEM((vectors, columns), BF16),
            pltpu.VMEM((nx, ka, 128), F32),
            pltpu.VMEM((nz, ka, 128), F32),
            pltpu.VMEM((nc, vectors // 2, 2 * vectors), F32),
            pltpu.VMEM((ny, vectors // 2, 2 * vectors), F32),
            pltpu.VMEM((na, ka, 128), F32),
            pltpu.VMEM((ny - 1, vectors, own), BF16),
            pltpu.VMEM((ny - 1, vectors, own), BF16),
            pltpu.VMEM((ny, vectors, own), BF16),
            pltpu.VMEM((ny, vectors, own), BF16),
            pltpu.VMEM((ny, vectors, own), F32),
            pltpu.VMEM((nc, 1, 128), F32),
            pltpu.VMEM((npairs * ny, 1, 128), F32),
            pltpu.SemaphoreType.DMA((nx, HALVES)),
            pltpu.SemaphoreType.DMA((2,)),
            pltpu.SemaphoreType.DMA((ny - 1,)),
            pltpu.SemaphoreType.DMA((ny,)),
            pltpu.SemaphoreType.DMA((11,)),
            pltpu.SemaphoreType.DMA((11,)),
        ],
        compiler_params=pltpu.CompilerParams(
            collective_id=0, has_side_effects=True, vmem_limit_bytes=60 * 1024 * 1024
        ),
        name="sigma_build",
    )(integrals, energy_gaps.reshape(1, rows), trial_vectors.T)
    sigma, subspace, residuals, norms = pl.pallas_call(
        put_out,
        out_shape=tuple(jax.ShapeDtypeStruct(s, F32) for s in shapes),
        in_specs=[vmem] * 4,
        out_specs=(hbm,) * 4,
        scratch_shapes=[pltpu.SemaphoreType.DMA((4,))],
        name="put_out",
    )(*[pltpu.with_memory_space_constraint(r, pltpu.VMEM) for r in results])
    return sigma.T, subspace, residuals.T, norms.reshape(vectors)


def solution(mesh):
    sizes = (8, 4, 4, 2)
    finer = Mesh(mesh.devices.reshape(sizes), AXES)
    return build(finer, sizes)


def build(finer, sizes):
    return jax.shard_map(
        functools.partial(local, sizes),
        mesh=finer,
        in_specs=(P(PAIR, AUX), P(PAIR), P(PAIR, None)),
        out_specs=(P(PAIR + AUX, None), P(), P(PAIR + AUX, None), P()),
        check_vma=False,
    )
```

```python
import functools

import jax
import jax.numpy as jnp
from jax import lax
from jax.experimental import pallas as pl
from jax.experimental.pallas import tpu as pltpu
from jax.sharding import Mesh
from jax.sharding import PartitionSpec as P

AXES = ("z", "x", "y", "c")
PAIR = ("z", "x")
AUX = ("y", "c")
EPSILON = 1e-06
PIECES = 4
HALVES = 4
F32 = jnp.float32
BF16 = jnp.bfloat16
NT = (((1,), (1,)), ((), ()))


def farthest(n):
    return sorted(range(n), key=lambda d: -min(d, n - d))


def far_first(i, n):
    step = lax.div(i + 1, 2)
    return n // 2 + step * (1 - 2 * lax.rem(i, 2))


def kernel(
    sizes,
    integrals,
    gaps,
    trial,
    sigma,
    subspace,
    residuals,
    norms,
    held,
    turned,
    v,
    g,
    vh,
    parts,
    parts_in,
    half,
    at,
    mx,
    mz,
    gc,
    gy,
    prows,
    terms,
    terms_in,
    chip_out,
    chip_in,
    coupled,
    nchip,
    nall,
    load_sem,
    small_load,
    terms_sem,
    chip_sem,
    send_sem,
    recv_sem,
):
    nz, nx, ny, nc = sizes
    na, npairs = ny * nc, nz * nx
    vectors, rows = v.shape
    columns = held.shape[1]
    kz, cx = vectors // nz, columns // nx
    own, ka = rows // na, vectors // na
    total_pairs = float(rows * npairs)
    z, x, y, c = (lax.axis_index(n) for n in AXES)
    a = y * nc + c
    me = z * nx + x

    zs, xs, ys, cs = ([lax.rem(p + d, n) for d in range(n)] for p, n in zip((z, x, y, c), sizes))
    plane = [(zs[i], xs[j], y, c) for i in farthest(nz) for j in farthest(nx)][:-1]
    group = [(z, x, ys[i], cs[j]) for i in farthest(ny) for j in reversed(range(nc))][:-1]
    sibling = (z, x, y, cs[1])
    y_others = [(z, x, ys[i], c) for i in farthest(ny)][:-1]
    x_others = [(z, xs[j], y, c) for j in farthest(nx)][:-1]
    z_others = [(zs[i], x, y, c) for i in farthest(nz)][:-1]

    def send(src, dst, k, to):
        pltpu.make_async_remote_copy(
            src_ref=src,
            dst_ref=dst,
            send_sem=send_sem.at[k],
            recv_sem=recv_sem.at[k],
            device_id=to,
            device_id_type=pl.DeviceIdType.MESH,
        ).start()

    def arrived(ref, k):
        pltpu.make_async_remote_copy(
            src_ref=ref,
            dst_ref=ref,
            send_sem=send_sem.at[k],
            recv_sem=recv_sem.at[k],
            device_id=sibling,
            device_id_type=pl.DeviceIdType.MESH,
        ).wait_recv()

    def sent(ref, k):
        pltpu.make_async_remote_copy(
            src_ref=ref,
            dst_ref=ref,
            send_sem=send_sem.at[k],
            recv_sem=recv_sem.at[k],
            device_id=sibling,
            device_id_type=pl.DeviceIdType.MESH,
        ).wait_send()

    def each(n, body):
        def step(i, carry):
            body(i)
            return carry

        lax.fori_loop(0, n, step, 0)

    load_v = pltpu.make_async_copy(trial, v, small_load.at[0])
    load_g = pltpu.make_async_copy(gaps, g, small_load.at[1])
    load_v.start()
    load_g.start()

    def columns_of(i):
        xx = lax.rem(x + far_first(i, nx), nx)
        return pl.ds(pl.multiple_of(xx * cx, 128), cx)

    piece = rows // PIECES

    def load_chunk(i):
        for p in range(PIECES):
            where = (pl.ds(p * piece, piece), columns_of(i))
            sem = load_sem.at[i, p * HALVES // PIECES]
            pltpu.make_async_copy(integrals.at[where], held.at[where], sem).start()

    load_chunk(0)
    barrier = pltpu.get_barrier_semaphore()
    for to in plane + group:
        pl.semaphore_signal(barrier, inc=1, device_id=to, device_id_type=pl.DeviceIdType.MESH)
    for i in range(1, nx):
        load_chunk(i)

    load_v.wait()
    load_g.wait()
    vh[...] = v[...].astype(BF16)

    def scatter(i):
        xx = lax.rem(x + far_first(i, nx), nx)
        for j, oz in enumerate(farthest(nz)[:-1]):
            send(parts.at[i, zs[oz]], parts_in.at[j * nx + i], 0, (zs[oz], xx, y, c))

        @pl.when(i < nx - 1)
        def _():
            send(parts.at[i, z], parts_in.at[(nz - 1) * nx + i], 0, (z, xx, y, c))

    def first_product(i):
        cols = columns_of(i)
        part = 0.0
        for h in range(HALVES):
            span = pl.ds(h * rows // HALVES, rows // HALVES)
            where = (span, cols)
            pltpu.make_async_copy(integrals.at[where], held.at[where], load_sem.at[i, h]).wait()
            part = part + jnp.dot(vh[:, span], held[where], preferred_element_type=F32)
        parts[i] = part.astype(BF16).reshape(nz, kz, cx)

        @pl.when(i == 1)
        def _():
            pl.semaphore_wait(barrier, len(plane) + len(group))
            scatter(0)

        @pl.when(i > 0)
        def _():
            scatter(i)

    each(nx, first_product)

    first = pl.multiple_of(a * ka, ka)
    mine = v[pl.ds(first, ka), :]
    gv = v[...] * g[...]
    m1 = lax.dot_general(mine, gv, NT, precision=lax.Precision.HIGHEST, preferred_element_type=F32)
    squares = jnp.sum(mine * mine, axis=1, keepdims=True)
    mx[x] = jnp.concatenate([m1, jnp.broadcast_to(squares, (ka, vectors))], axis=1)
    for to in x_others:
        send(mx.at[x], mx.at[x], 1, to)

    def turn(i):
        block = pl.ds(pl.multiple_of(i * 128, 128), 128)
        turned[:, block] = held[block, :].T

    each(rows // 256, turn)

    arrived(mx.at[pl.ds(0, nx - 1)], 1)
    mz[z] = jnp.sum(mx[...], axis=0)
    for to in z_others:
        send(mz.at[z], mz.at[z], 3, to)

    arrived(parts_in, 0)
    block = parts[nx - 1, z].astype(F32)
    block = block + jnp.sum(parts_in[...].astype(F32), axis=0)
    slot = x * nz + z
    half[slot] = block.astype(BF16)
    for to in plane:
        send(half.at[slot], half.at[slot], 2, to)

    each(rows // 256, lambda i: turn(rows // 256 + i))

    arrived(mz.at[pl.ds(0, nz - 1)], 3)
    prows[a] = jnp.sum(mz[...], axis=0)
    for to in group:
        send(prows.at[a], prows.at[a], 6, to)

    arrived(half.at[pl.ds(0, npairs - 1)], 2)
    for i in range(nx):
        at[:, i * cx : (i + 1) * cx] = half[i * nz : (i + 1) * nz].reshape(vectors, cx)

    low = vectors // 2
    gram = lax.dot_general(at[...], at[...], NT, preferred_element_type=F32)
    gc[c] = jnp.concatenate([gram[:low], gram[low:]], axis=1)
    send(gc.at[c], gc.at[c], 4, sibling)

    def share_gram():
        arrived(gc.at[0], 4)
        gy[y] = gc[0] + gc[1]
        for to in y_others:
            send(gy.at[y], gy.at[y], 7, to)

    @pl.when(c == 0)
    def _():
        share_gram()

    def pass_on(i):
        pltpu.make_async_remote_copy(
            src_ref=chip_out.at[i],
            dst_ref=chip_in.at[i],
            send_sem=send_sem.at[10],
            recv_sem=chip_sem.at[i],
            device_id=sibling,
            device_id_type=pl.DeviceIdType.MESH,
        ).wait_recv()
        whole = coupled[i] + chip_in[i].astype(F32)

        @pl.when(i < ny - 1)
        def _():
            terms[i] = whole.astype(BF16)
            pltpu.make_async_remote_copy(
                src_ref=terms.at[i],
                dst_ref=terms_in.at[i],
                send_sem=send_sem.at[5],
                recv_sem=terms_sem.at[i],
                device_id=(z, x, lax.rem(y + far_first(i, ny), ny), c),
                device_id_type=pl.DeviceIdType.MESH,
            ).start()

        @pl.when(i == ny - 1)
        def _():
            coupled[i] = whole

    def second_product(i):
        yy = lax.rem(y + far_first(i, ny), ny)
        begin = pl.multiple_of(yy * nc * own, 128)
        out = jnp.dot(at[...], turned[:, pl.ds(begin, nc * own)], preferred_element_type=F32)
        theirs = jnp.where(c == 0, out[:, own:], out[:, :own])
        chip_out[i] = theirs.astype(BF16)
        pltpu.make_async_remote_copy(
            src_ref=chip_out.at[i],
            dst_ref=chip_in.at[i],
            send_sem=send_sem.at[10],
            recv_sem=chip_sem.at[i],
            device_id=sibling,
            device_id_type=pl.DeviceIdType.MESH,
        ).start()
        coupled[i] = jnp.where(c == 0, out[:, :own], out[:, own:])

        @pl.when(c == 0)
        def _():
            pass_on(i)

    each(ny, second_product)

    @pl.when(c > 0)
    def _():
        share_gram()
        each(ny, pass_on)

    mine_at = pl.ds(pl.multiple_of(a * own, 128), own)
    own_trial = v[:, mine_at]

    arrived(prows.at[pl.ds(0, na - 1)], 6)
    arrived(gy.at[pl.ds(0, ny - 1)], 7)
    gram = jnp.sum(gy[...], axis=0)
    gram = jnp.concatenate([gram[:, :vectors], gram[:, vectors:]], axis=0)
    inputs = prows[...].reshape(vectors, 2 * vectors)
    sub = (inputs[:, :vectors] + 2.0 * gram) / total_pairs
    row = lax.broadcasted_iota(jnp.int32, (vectors, vectors), 0)
    lane = lax.broadcasted_iota(jnp.int32, (vectors, vectors), 1)
    diagonal = jnp.sum(jnp.where(row == lane, sub, 0.0), axis=1, keepdims=True)
    intersection = inputs[:, vectors : vectors + 1] / total_pairs
    rayleigh = diagonal / (intersection + EPSILON)
    subspace[...] = sub

    total = coupled[ny - 1]
    for i in range(ny - 1):
        pltpu.make_async_remote_copy(
            src_ref=terms.at[i],
            dst_ref=terms_in.at[i],
            send_sem=send_sem.at[5],
            recv_sem=terms_sem.at[i],
            device_id=sibling,
            device_id_type=pl.DeviceIdType.MESH,
        ).wait_recv()
        total = total + terms_in[i].astype(F32)

    sigma_own = own_trial * g[:, mine_at] + 2.0 * total
    sigma[...] = sigma_own
    residual = sigma_own - rayleigh * own_trial
    residuals[...] = residual
    squared = residual * residual
    lanes = squared[:, :128]
    for i in range(1, own // 128):
        lanes = lanes + squared[:, i * 128 : (i + 1) * 128]
    lanes = jnp.concatenate([lanes, jnp.zeros((128 - vectors, 128), F32)], axis=0)
    nchip[c] = jnp.sum(lanes.T, axis=0, keepdims=True)
    send(nchip.at[c], nchip.at[c], 8, sibling)

    arrived(nchip.at[0], 8)
    nall[me * ny + y] = nchip[0] + nchip[1]

    def share(t):
        zz = lax.rem(z + far_first(t, nz), nz)
        spots = [(zz, xs[j], ys[k], c) for j in farthest(nx) for k in farthest(ny)]
        for to in spots[:-1]:
            send(nall.at[me * ny + y], nall.at[me * ny + y], 9, to)

        @pl.when(t < nz - 1)
        def _():
            send(nall.at[me * ny + y], nall.at[me * ny + y], 9, spots[-1])

    each(nz, share)

    sent(parts_in, 0)
    sent(mx.at[pl.ds(0, nx - 1)], 1)
    sent(half.at[pl.ds(0, npairs - 1)], 2)
    sent(mz.at[pl.ds(0, nz - 1)], 3)
    sent(gc.at[0], 4)
    sent(terms, 5)
    sent(chip_out, 10)
    sent(prows.at[pl.ds(0, na - 1)], 6)
    sent(gy.at[pl.ds(0, ny - 1)], 7)
    sent(nchip.at[0], 8)

    arrived(nall.at[pl.ds(0, npairs * ny - 1)], 9)
    sent(nall.at[pl.ds(0, npairs * ny - 1)], 9)
    total = jnp.sum(nall[...], axis=0) / total_pairs
    norms[...] = jnp.sqrt(total[:, :vectors] + EPSILON)


def put_out(*refs):
    copies = [pltpu.make_async_copy(refs[i], refs[4 + i], refs[8].at[i]) for i in range(4)]
    for copy in copies:
        copy.start()
    for copy in copies:
        copy.wait()


def local(sizes, integrals, energy_gaps, trial_vectors):
    nz, nx, ny, nc = sizes
    na, npairs = ny * nc, nz * nx
    rows, columns = integrals.shape
    vectors = trial_vectors.shape[1]
    kz, cx = vectors // nz, columns // nx
    own, ka = rows // na, vectors // na
    hbm = pl.BlockSpec(memory_space=pl.ANY)
    vmem = pl.BlockSpec(memory_space=pltpu.VMEM)
    shapes = ((vectors, own), (vectors, vectors), (vectors, own), (1, vectors))
    results = pl.pallas_call(
        functools.partial(kernel, sizes),
        out_shape=tuple(pltpu.VMEM(s, F32) for s in shapes),
        in_specs=[hbm, hbm, hbm],
        out_specs=(vmem,) * 4,
        scratch_shapes=[
            pltpu.VMEM((rows, columns), BF16),
            pltpu.VMEM((columns, rows), BF16),
            pltpu.VMEM((vectors, rows), F32),
            pltpu.VMEM((1, rows), F32),
            pltpu.VMEM((vectors, rows), BF16),
            pltpu.VMEM((nx, nz, kz, cx), BF16),
            pltpu.VMEM((npairs - 1, kz, cx), BF16),
            pltpu.VMEM((npairs, kz, cx), BF16),
            pltpu.VMEM((vectors, columns), BF16),
            pltpu.VMEM((nx, ka, 128), F32),
            pltpu.VMEM((nz, ka, 128), F32),
            pltpu.VMEM((nc, vectors // 2, 2 * vectors), F32),
            pltpu.VMEM((ny, vectors // 2, 2 * vectors), F32),
            pltpu.VMEM((na, ka, 128), F32),
            pltpu.VMEM((ny - 1, vectors, own), BF16),
            pltpu.VMEM((ny - 1, vectors, own), BF16),
            pltpu.VMEM((ny, vectors, own), BF16),
            pltpu.VMEM((ny, vectors, own), BF16),
            pltpu.VMEM((ny, vectors, own), F32),
            pltpu.VMEM((nc, 1, 128), F32),
            pltpu.VMEM((npairs * ny, 1, 128), F32),
            pltpu.SemaphoreType.DMA((nx, HALVES)),
            pltpu.SemaphoreType.DMA((2,)),
            pltpu.SemaphoreType.DMA((ny - 1,)),
            pltpu.SemaphoreType.DMA((ny,)),
            pltpu.SemaphoreType.DMA((11,)),
            pltpu.SemaphoreType.DMA((11,)),
        ],
        compiler_params=pltpu.CompilerParams(
            collective_id=0, has_side_effects=True, vmem_limit_bytes=60 * 1024 * 1024
        ),
        name="sigma_build",
    )(integrals, energy_gaps.reshape(1, rows), trial_vectors.T)
    sigma, subspace, residuals, norms = pl.pallas_call(
        put_out,
        out_shape=tuple(jax.ShapeDtypeStruct(s, F32) for s in shapes),
        in_specs=[vmem] * 4,
        out_specs=(hbm,) * 4,
        scratch_shapes=[pltpu.SemaphoreType.DMA((4,))],
        name="put_out",
    )(*[pltpu.with_memory_space_constraint(r, pltpu.VMEM) for r in results])
    return sigma.T, subspace, residuals.T, norms.reshape(vectors)


def solution(mesh):
    sizes = (8, 4, 4, 2)
    finer = Mesh(mesh.devices.reshape(sizes), AXES)
    return build(finer, sizes)


def build(finer, sizes):
    return jax.shard_map(
        functools.partial(local, sizes),
        mesh=finer,
        in_specs=(P(PAIR, AUX), P(PAIR), P(PAIR, None)),
        out_specs=(P(PAIR + AUX, None), P(), P(PAIR + AUX, None), P()),
        check_vma=False,
    )
```
